32 devices in a mesh: slab: 8 (over z, x), rhs: 4 (over y, core).
Axes of the slice: x: 2, y: 2, z: 4, core: 2. Of those that a mesh axis runs over, the one named last changes fastest.
Arguments:
- targets: float32 [8, 128, 256], P('rhs', 'slab'), may hold values from -60 to 60
- counts: int32 [128], P('slab'), may hold values from 1 to 256, 20480 in all
- cell_rows: int32 [128, 256], P('slab'), may hold values from 0 to 255
- cell_cols: int32 [128, 256], P('slab'), may hold values from 0 to 127
- fractions: float32 [2, 128, 256], P(None, 'slab'), may hold values from 0 to 1
- spectrum: float32 [2048, 2048], P(None, ('slab', 'rhs')), may hold values from 0.25 to 4, as said below
- noise_var: float32 [1], replicated, may hold values from 0.1 to 1
Outputs:
- solution: float32 [8, 128, 256], P('rhs', 'slab')
- residual: float32 [8, 128, 256], P('rhs', 'slab')
The draws below stay inside these ranges and needn't reach their ends.
Inputs may be any that keep to these rules, and one draw needn't show every extreme that they name: Each tile has 256 slots; tile t holds points in its first counts[t] slots, and the other slots are empty: their entries are ignored and their outputs are zero. Even in frequency: spectrum[a, b] = spectrum[(2048 - a) % 2048, (2048 - b) % 2048].
All inputs are finite; a program needn't handle non-finite values. No bound on the sum of `counts` on one device may be relied on, other than what follows from the above.
Results may differ from the reference program's by a relative error of at most 0.0002.
Values sent between devices are 32-bit elements; how exact they have to be, the bound alone decides.
A program may use at most 128 MiB of HBM per device.

```python
import math
import jax
import jax.numpy as jnp
import numpy as np
from jax import lax

G = 2048
TC = 128
CAP = 256
RHS = 8
ITERS = 2
ROWS_DEV = 256
TILES = 16
TILES_ALL = 128


def draw_targets(key, part):
    position = jnp.arange(TILES_ALL, dtype=jnp.float32) / TILES_ALL
    growth = jnp.exp(jnp.log(3.0) * position)[None, :, None]
    values = jax.random.normal(key, (RHS, TILES_ALL, CAP), jnp.float32) * growth
    return jnp.clip(values, -60.0, 60.0)


def draw_spectrum(key, part):
    values = jnp.exp(jax.random.uniform(key, (G, G), jnp.float32, math.log(0.25), math.log(4.0)))
    mirrored = jnp.roll(jnp.flip(values, (0, 1)), 1, (0, 1))
    return jnp.clip(0.5 * (values + mirrored), 0.25, 4.0)


def plant(array, stream_key, low, top_value):
    longest = array.shape.index(max(array.shape))
    spots = []
    for shift in (0, 1):
        where = [jax.random.randint(jax.random.fold_in(stream_key, axis), (), 0, length) for axis, length in enumerate(array.shape)]
        where[longest] = (where[longest] + shift) % array.shape[longest]
        spots.append(tuple(where))
    return array.at[spots[0]].set(low).at[spots[1]].set(top_value)


def levels(own_key, dims, pieces, low, top_value):
    loudness, own = 1.0, jax.random.fold_in(own_key, 6)
    for dim, blocks in pieces:
        steps = jnp.exp(jax.random.uniform(jax.random.fold_in(own, dim), (blocks,), jnp.float32, low / len(pieces), top_value / len(pieces)))
        loudness = loudness * jnp.repeat(steps, dims[dim] // blocks).reshape([-1 if axis == dim else 1 for axis in range(len(dims))])
    return loudness


def split_up(amount, total, bound, lean):
    portions = [(1 << 20) // math.isqrt(grade ** lean) + 1 for grade in range(2, amount + 1)]
    spare, given = total - bound - (amount - 1), [1] * (amount - 1)
    while spare > 0:
        free = [i for i in range(amount - 1) if given[i] < bound]
        mass, remaining = sum([portions[i] for i in free]), spare
        for i in free:
            more = min(bound - given[i], max(1, remaining * portions[i] // mass), spare)
            given[i] = given[i] + more
            spare = spare - more
    return np.array([bound] + given)


def uneven(stream_key, amount, total, most, slope):
    if amount == 2:
        one = jax.random.randint(stream_key, (), max(1, total - most), min(most, total - 1) + 1)
        return jnp.stack([one, total - one])
    sizes = jnp.asarray(split_up(amount, total, most, slope), jnp.int32)
    twos = (amount - 1) // 2
    giver, sink = sizes[1:1 + 2 * twos:2], sizes[2:2 + 2 * twos:2]
    slack = jnp.minimum(giver - 1, most - sink)
    moved = jax.random.randint(jax.random.fold_in(stream_key, 1), (twos,), 0, 1 << 20) % (slack + 1)
    sizes = sizes.at[1:1 + 2 * twos:2].set(giver - moved).at[2:2 + 2 * twos:2].set(sink + moved)
    return sizes[jax.random.permutation(jax.random.fold_in(stream_key, 2), amount)]


def setup_inputs(seed: int = 0) -> dict:
    splits = jax.random.split(jax.random.key(seed), 8)
    return {
        "targets": draw_targets(jax.random.fold_in(splits[7], 71), 0),
        "counts": uneven(splits[1], TILES_ALL, TILES_ALL * CAP * 5 // 8, CAP, 2).astype(jnp.int32),
        "cell_rows": plant(jax.random.randint(splits[2], (TILES_ALL, CAP), 0, ROWS_DEV), jax.random.fold_in(splits[2], 1), 0, ROWS_DEV - 1).astype(jnp.int32),
        "cell_cols": plant(jax.random.randint(splits[3], (TILES_ALL, CAP), 0, TC), jax.random.fold_in(splits[3], 1), 0, TC - 1).astype(jnp.int32),
        "fractions": jnp.clip(1.0 * jax.random.uniform(splits[4], (2, TILES_ALL, CAP), jnp.float32) ** levels(splits[4], (2, TILES_ALL, CAP), ((1, 8),), -0.2, 0.2), 0.0, 1.0),
        "spectrum": draw_spectrum(jax.random.fold_in(splits[7], 71), 0),
        "noise_var": jnp.clip(jnp.exp(jax.random.uniform(splits[6], (1,), jnp.float32, math.log(0.1), math.log(1.0))), 0.1, 1.0),
    }


def cubic_weights(fraction):
    return (((-0.5 * fraction + 1.0) * fraction - 0.5) * fraction,
            (1.5 * fraction - 2.5) * fraction * fraction + 1.0,
            ((-1.5 * fraction + 2.0) * fraction + 0.5) * fraction,
            (0.5 * fraction - 0.5) * fraction * fraction)


def stencil(counts, cell_rows, cell_cols, fractions):
    tile_ids = jnp.arange(TILES_ALL, dtype=jnp.int32)
    row_base = (tile_ids // TILES) * ROWS_DEV
    col_base = (tile_ids % TILES) * TC
    grid_rows = row_base[:, None] + cell_rows
    grid_cols = col_base[:, None] + cell_cols
    slot_ids = jnp.arange(CAP, dtype=jnp.int32)
    live = (slot_ids[None, :] < counts[:, None]).astype(jnp.float32)
    row_weights = cubic_weights(fractions[0])
    col_weights = cubic_weights(fractions[1])
    indices = []
    weights = []
    for row_shift in range(4):
        for col_shift in range(4):
            rows_at = (grid_rows - 1 + row_shift) % G
            cols_at = (grid_cols - 1 + col_shift) % G
            indices.append((rows_at * G + cols_at).astype(jnp.int32).reshape(-1))
            weights.append(row_weights[row_shift] * col_weights[col_shift])
    return live, indices, weights


def kernel_product(grid_field, spectrum):
    return jnp.real(jnp.fft.ifft2(spectrum * jnp.fft.fft2(grid_field))).astype(jnp.float32)


def apply_operator(vector, live, indices, weights, spectrum, noise_var):
    grid_flat = jnp.zeros((RHS, G * G), jnp.float32)
    for flat_index, weight in zip(indices, weights):
        grid_flat = grid_flat.at[:, flat_index].add((weight[None] * vector).reshape(RHS, -1))
    grid = grid_flat.reshape(RHS, G, G)
    smoothed = lax.map(lambda grid_field: kernel_product(grid_field, spectrum), grid)
    smooth_flat = smoothed.reshape(RHS, G * G)
    result = jnp.zeros(vector.shape, jnp.float32)
    for flat_index, weight in zip(indices, weights):
        picked = jnp.take(smooth_flat, flat_index, axis=1).reshape(vector.shape)
        result = result + weight[None] * picked
    return live[None] * result + noise_var[0] * vector


def reference(targets, counts, cell_rows, cell_cols, fractions, spectrum, noise_var):
    live, indices, weights = stencil(counts, cell_rows, cell_cols, fractions)
    residual = live[None] * targets
    direction = residual
    solution = jnp.zeros(residual.shape, jnp.float32)
    norm_now = jnp.sum(residual * residual, axis=(1, 2))
    for repeat in range(ITERS):
        image = apply_operator(direction, live, indices, weights, spectrum, noise_var)
        alpha = norm_now / jnp.sum(direction * image, axis=(1, 2))
        solution = solution + alpha[:, None, None] * direction
        residual = residual - alpha[:, None, None] * image
        if repeat + 1 < ITERS:
            norm_next = jnp.sum(residual * residual, axis=(1, 2))
            direction = residual + (norm_next / norm_now)[:, None, None] * direction
            norm_now = norm_next
    return solution, residual
```

```python
import functools
import math

import jax
import jax.numpy as jnp
import numpy as np
from jax import lax
from jax.experimental import pallas as pl
from jax.experimental.pallas import tpu as pltpu
from jax.sharding import PartitionSpec as P

G = 2048
TC = 128
ITERS = 2
RADIX = 8
LONG = G // RADIX
RIM = 8
PARTS = 2
F32 = jnp.float32
BF16 = jnp.bfloat16


def cubic_weights(fraction):
    return (
        ((-0.5 * fraction + 1.0) * fraction - 0.5) * fraction,
        (1.5 * fraction - 2.5) * fraction * fraction + 1.0,
        ((-1.5 * fraction + 2.0) * fraction + 0.5) * fraction,
        (0.5 * fraction - 0.5) * fraction * fraction,
    )


def stencil_table(cell, fraction, extent):
    weights = cubic_weights(fraction)
    position = lax.broadcasted_iota(jnp.int32, (extent, cell.shape[1]), 0)
    table = jnp.zeros((extent, cell.shape[1]), F32)
    for offset in range(4):
        target = cell + (offset - 1)
        target = jnp.where(target < 0, extent - 1, target)
        table = jnp.where(position == target, weights[offset], table)
    return table


def halves(value):
    high = value.astype(BF16)
    return high, (value - high.astype(F32)).astype(BF16)


def dot_pieces(left, right, dims=(((1,), (0,)), ((), ()))):
    dot = functools.partial(lax.dot_general, dimension_numbers=dims, preferred_element_type=F32)
    return dot(left[0], right[0]) + (dot(left[0], right[1]) + dot(left[1], right[0]))


def add(a, b):
    return (a[0] + b[0], a[1] + b[1])


def sub(a, b):
    return (a[0] - b[0], a[1] - b[1])


def quarter(a, sign):
    return (-sign * a[1], sign * a[0])


def dft4(x, sign):
    p, m = add(x[0], x[2]), sub(x[0], x[2])
    q, n = add(x[1], x[3]), quarter(sub(x[1], x[3]), sign)
    return [add(p, q), add(m, n), sub(p, q), sub(m, n)]


def dft8(x, sign):
    even, odd = dft4(x[0::2], sign), dft4(x[1::2], sign)
    r = math.sqrt(0.5)
    a, c = odd[1], odd[3]
    odd = [
        odd[0],
        (r * (a[0] - sign * a[1]), r * (a[1] + sign * a[0])),
        quarter(odd[2], sign),
        (r * (-c[0] - sign * c[1]), r * (-c[1] + sign * c[0])),
    ]
    return [add(e, o) for e, o in zip(even, odd)] + [sub(e, o) for e, o in zip(even, odd)]


def spread_kernel(vec, rows, cols, frac, trig_hi, trig_lo, twist, *rest):
    outs, (field, mixed) = rest[:PARTS], rest[PARTS:]
    tiles, ext = field.shape[1], field.shape[2]
    count = outs[0].shape[0]
    width = outs[0].shape[2] // 2
    share = count // RADIX
    field[...] = jnp.zeros_like(field)

    def one_tile(t, carry):
        row_tab = stencil_table(rows[pl.ds(t, 1), :], frac[0, pl.ds(t, 1), :], ext)
        col_tab = stencil_table(cols[pl.ds(t, 1), :], frac[1, pl.ds(t, 1), :], 2 * TC)
        weighted = jnp.concatenate(
            [row_tab * vec[0, pl.ds(t, 1), :], row_tab * vec[1, pl.ds(t, 1), :]], axis=0
        )
        piece = dot_pieces(halves(weighted), halves(col_tab), (((1,), (1,)), ((), ())))
        after = lax.rem(t + 1, tiles)
        before = lax.rem(t + tiles - 1, tiles)
        low = lax.broadcasted_iota(jnp.int32, (ext, TC), 1) < TC // 2
        for k in range(2):
            block = piece[k * ext : (k + 1) * ext]
            rim = block[:, TC:]
            field[k, t] = field[k, t] + block[:, :TC]
            field[k, after] = field[k, after] + jnp.where(low, rim, 0.0)
            field[k, before] = field[k, before] + jnp.where(low, 0.0, rim)
        return carry

    lax.fori_loop(0, tiles, one_tile, 0)

    def one_strip(i, carry):
        strip = pl.ds(pl.multiple_of(i * 8, 8), 8)
        for h in range(LONG // TC):
            lanes = slice(h * TC, (h + 1) * TC)
            x = [
                (field[0, j * (LONG // TC) + h, strip, :], field[1, j * (LONG // TC) + h, strip, :])
                for j in range(RADIX)
            ]
            for d, (re, im) in enumerate(dft8(x, -1.0)):
                c = twist[d : d + 1, lanes]
                s = twist[RADIX + d : RADIX + d + 1, lanes]
                mixed[d, 0, strip, lanes] = re * c - im * s
                mixed[d, 1, strip, lanes] = re * s + im * c
        return carry

    lax.fori_loop(0, ext // 8, one_strip, 0)
    table = (trig_hi[...], trig_lo[...])
    for d in range(RADIX):
        x = jnp.concatenate([mixed[d, 0], mixed[d, 1]], axis=0)
        y = dot_pieces(halves(x), table)
        re = y[:ext, :LONG] - y[ext:, LONG:]
        im = y[ext:, :LONG] + y[:ext, LONG:]
        for i in range(share):
            for h in range(PARTS):
                start = (i * PARTS + h) * width
                outs[h][d * share + i, :, :width] = re[:, start : start + width]
                outs[h][d * share + i, :, width:] = im[:, start : start + width]


def middle_kernel(part, ext_in, spectrum, trig_hi, trig_lo, twist, ext_out, grid, mixed):
    count, ext, both = ext_in.shape
    width = both // 2
    rows = ext - RIM
    for s in range(count):
        grid[s * rows : (s + 1) * rows] = ext_in[s, :rows]
    upper = lax.broadcasted_iota(jnp.int32, (RIM, both), 0) < RIM // 2
    for s in range(count):
        rim = ext_in[s, rows:]
        after = (s + 1) % count * rows
        before = ((s + count - 1) % count + 1) * rows - RIM
        grid[after : after + RIM] = grid[after : after + RIM] + jnp.where(upper, rim, 0.0)
        grid[before : before + RIM] = grid[before : before + RIM] + jnp.where(upper, 0.0, rim)

    def forward(i, carry):
        start = pl.multiple_of(i * 8, 8)
        x = []
        for j in range(RADIX):
            strip = pl.ds(pl.multiple_of(j * LONG + start, 8), 8)
            x.append((grid[strip, :width], grid[strip, width:]))
        for e, (re, im) in enumerate(dft8(x, -1.0)):
            c = twist[pl.ds(start, 8), e : e + 1]
            s = twist[pl.ds(start, 8), RADIX + e : RADIX + e + 1]
            mixed[e, pl.ds(start, 8), :width] = re * c - im * s
            mixed[e, pl.ds(start, 8), width:] = re * s + im * c
        return carry

    lax.fori_loop(0, LONG // 8, forward, 0)
    table = (trig_hi[...], trig_lo[...])
    scale = 1.0 / (G * G)
    for e in range(RADIX):
        y = dot_pieces(table, halves(mixed[e]))
        factor = spectrum[e, :, part * width : (part + 1) * width] * scale
        re = (y[:LONG, :width] - y[LONG:, width:]) * factor
        im = (y[:LONG, width:] + y[LONG:, :width]) * factor
        y = dot_pieces(table, halves(jnp.concatenate([re, im], axis=1)))
        re = y[:LONG, :width] + y[LONG:, width:]
        im = y[:LONG, width:] - y[LONG:, :width]
        c = twist[:, e : e + 1]
        s = twist[:, RADIX + e : RADIX + e + 1]
        mixed[e, :, :width] = re * c + im * s
        mixed[e, :, width:] = im * c - re * s

    def backward(i, carry):
        start = pl.multiple_of(i * 8, 8)
        strip = pl.ds(start, 8)
        x = [(mixed[e, strip, :width], mixed[e, strip, width:]) for e in range(RADIX)]
        for j, (re, im) in enumerate(dft8(x, 1.0)):
            out = pl.ds(pl.multiple_of(j * LONG + start, 8), 8)
            grid[out, :width] = re
            grid[out, width:] = im
        return carry

    lax.fori_loop(0, LONG // 8, backward, 0)
    for s in range(count):
        ext_out[s, :rows] = grid[s * rows : (s + 1) * rows]
        after = (s + 1) % count * rows
        before = ((s + count - 1) % count + 1) * rows - RIM
        ext_out[s, rows:] = jnp.where(
            upper, grid[after : after + RIM], grid[before : before + RIM]
        )


def gather_kernel(rows, cols, frac, trig_hi, trig_lo, twist, *rest):
    ins, out, (field, mixed) = rest[:PARTS], rest[PARTS], rest[PARTS + 1 :]
    tiles, ext = field.shape[1], field.shape[2]
    count = ins[0].shape[0]
    width = ins[0].shape[2] // 2
    share = count // RADIX
    table = (trig_hi[...], trig_lo[...])
    for d in range(RADIX):
        blocks = [(d * share + i, h) for i in range(share) for h in range(PARTS)]
        re = jnp.concatenate([ins[h][b, :, :width] for b, h in blocks], axis=1)
        im = jnp.concatenate([ins[h][b, :, width:] for b, h in blocks], axis=1)
        y = dot_pieces(halves(jnp.concatenate([re, im], axis=0)), table)
        re = y[:ext, :LONG] + y[ext:, LONG:]
        im = y[ext:, :LONG] - y[:ext, LONG:]
        c = twist[d : d + 1, :]
        s = twist[RADIX + d : RADIX + d + 1, :]
        mixed[d, 0] = re * c + im * s
        mixed[d, 1] = im * c - re * s

    def one_strip(i, carry):
        strip = pl.ds(pl.multiple_of(i * 8, 8), 8)
        for h in range(LONG // TC):
            lanes = slice(h * TC, (h + 1) * TC)
            x = [(mixed[d, 0, strip, lanes], mixed[d, 1, strip, lanes]) for d in range(RADIX)]
            for j, (re, im) in enumerate(dft8(x, 1.0)):
                field[0, j * (LONG // TC) + h, strip, :] = re
                field[1, j * (LONG // TC) + h, strip, :] = im
        return carry

    lax.fori_loop(0, ext // 8, one_strip, 0)

    def one_tile(t, carry):
        row_tab = stencil_table(rows[pl.ds(t, 1), :], frac[0, pl.ds(t, 1), :], ext)
        col_tab = stencil_table(cols[pl.ds(t, 1), :], frac[1, pl.ds(t, 1), :], 2 * TC)
        after = lax.rem(t + 1, tiles)
        before = lax.rem(t + tiles - 1, tiles)
        low = lax.broadcasted_iota(jnp.int32, (ext, TC), 1) < TC // 2
        near = jnp.concatenate(
            [
                jnp.concatenate(
                    [field[k, t], jnp.where(low, field[k, after], field[k, before])], axis=1
                )
                for k in range(2)
            ],
            axis=0,
        )
        blended = dot_pieces(halves(near), halves(col_tab))
        for k in range(2):
            value = jnp.sum(row_tab * blended[k * ext : (k + 1) * ext], axis=0, keepdims=True)
            out[k, pl.ds(t, 1), :] = value
        return carry

    lax.fori_loop(0, tiles, one_tile, 0)


def split_table(table):
    high = table.astype(np.float32).astype(BF16)
    low = (table - high.astype(np.float64)).astype(np.float32).astype(BF16)
    return jnp.asarray(high), jnp.asarray(low)


def column_order(share, count, ranks, width):
    kept = width // (RADIX * share)
    order = [
        (width // RADIX) * (ranks * s + r) + i * kept + k
        for i in range(share)
        for r in range(ranks)
        for s in range(count)
        for k in range(kept)
    ]
    return np.array(order)


def exchanged_spectrum(spectrum, count, ranks):
    share = count // RADIX
    width = spectrum.shape[1]
    late = width % (RADIX * share) == 0
    if not late:
        spectrum = lax.all_gather(spectrum, "rhs", axis=1, tiled=True)
        width = spectrum.shape[1]
        ranks = 1
    kept = width // (RADIX * share)
    turned = spectrum.T.reshape(share, kept, RADIX, G).transpose(2, 0, 1, 3)
    turned = lax.all_to_all(turned.reshape(count, kept, G), "slab", 0, 0, tiled=True)
    turned = turned.reshape(count * kept, G)
    if late:
        turned = lax.all_gather(turned, "rhs", axis=0, tiled=True)
    by_residue = turned.T.reshape(LONG, RADIX, -1).transpose(1, 0, 2)
    return by_residue, column_order(share, count, ranks, width)


def total(partial):
    return jnp.sum(lax.all_gather(partial, "slab"), axis=0)


def per_device(targets, counts, cell_rows, cell_cols, fractions, spectrum, noise_var):
    tiles, capacity = cell_rows.shape
    count = lax.axis_size("slab")
    ranks = lax.axis_size("rhs")
    rows_dev = G // count
    ext = rows_dev + RIM
    width = G // count // PARTS
    both = 2 * width
    block = jax.ShapeDtypeStruct((count, ext, both), F32)

    factors, order = exchanged_spectrum(spectrum, count, ranks)
    short = np.arange(LONG)
    angle = (short[:, None] * order[None, :] % LONG) * (2.0 * np.pi / LONG)
    forth = split_table(np.concatenate([np.cos(angle), -np.sin(angle)], axis=1))
    back = split_table(np.concatenate([np.cos(angle).T, -np.sin(angle).T], axis=1))
    angle = (short[:, None] * short[None, :] % LONG) * (2.0 * np.pi / LONG)
    inner = split_table(np.concatenate([np.cos(angle), -np.sin(angle)], axis=0))
    angle = np.arange(RADIX)[:, None] * short[None, :] * (2.0 * np.pi / G)
    twist = np.concatenate([np.cos(angle), -np.sin(angle)], axis=0).astype(np.float32)
    twist_rows, twist_cols = jnp.asarray(twist.T), jnp.asarray(twist)
    scratch = [
        pltpu.VMEM((2, tiles, ext, TC), F32),
        pltpu.VMEM((RADIX, 2, ext, LONG), F32),
    ]

    slot_index = lax.broadcasted_iota(jnp.int32, (tiles, capacity), 1)
    live = (slot_index < counts[:, None]).astype(F32)

    def smoothed(direction):
        sent = pl.pallas_call(
            spread_kernel, out_shape=[block] * PARTS, scratch_shapes=scratch, name="spread"
        )(direction, cell_rows, cell_cols, fractions, *forth, twist_cols)
        returned = []
        for part in range(PARTS):
            there = lax.all_to_all(sent[part], "slab", 0, 0, tiled=True)
            weighed = pl.pallas_call(
                functools.partial(middle_kernel, part),
                out_shape=block,
                scratch_shapes=[
                    pltpu.VMEM((G, both), F32),
                    pltpu.VMEM((RADIX, LONG, both), F32),
                ],
                name="middle",
            )(there, factors, *inner, twist_rows)
            returned.append(lax.all_to_all(weighed, "slab", 0, 0, tiled=True))
        return pl.pallas_call(
            gather_kernel,
            out_shape=jax.ShapeDtypeStruct(direction.shape, F32),
            scratch_shapes=scratch,
            name="gather",
        )(cell_rows, cell_cols, fractions, *back, twist_cols, *returned)

    residual = live[None] * targets
    solution = jnp.zeros(residual.shape, F32)
    direction = residual
    norm_now = total(jnp.sum(residual * residual, axis=(1, 2)))
    for repeat in range(ITERS):
        image = live[None] * smoothed(direction) + noise_var[0] * direction
        product = total(jnp.sum(direction * image, axis=(1, 2)))
        alpha = (norm_now / product)[:, None, None]
        solution = solution + alpha * direction
        residual = residual - alpha * image
        if repeat + 1 < ITERS:
            norm_next = total(jnp.sum(residual * residual, axis=(1, 2)))
            direction = residual + (norm_next / norm_now)[:, None, None] * direction
            norm_now = norm_next
    return (solution, residual)


def solution(mesh):
    placed = (
        P("rhs", "slab", None),
        P("slab"),
        P("slab", None),
        P("slab", None),
        P(None, "slab", None),
        P(None, ("slab", "rhs")),
        P(),
    )
    return jax.shard_map(
        per_device,
        mesh=mesh,
        in_specs=placed,
        out_specs=(P("rhs", "slab", None), P("rhs", "slab", None)),
        check_vma=False,
    )
```
